32 devices in a mesh: grp: 4 (over y, x), own: 8 (over z, core).
Axes of the slice: x: 2, y: 2, z: 4, core: 2. Of those that a mesh axis runs over, the one named last changes fastest.
Arguments:
- tile_row: int32 [4, 8, 1536], P('grp', 'own'), may hold values from 0 to 7
- pixel_col: int32 [4, 8, 1536], P('grp', 'own'), may hold values from 0 to 16383
- weight: bfloat16 [4, 8, 1536], P('grp', 'own'), may hold values from 0.25 to 4
- counts: int32 [4, 8, 8], P('grp', 'own'), may hold values from 1 to 192
- kernel: float32 [9, 9], replicated, may hold values from 0.01 to 0.05
Outputs:
- smoothed: float32 [64, 16384], P('own', 'grp')
The draws below stay inside these ranges and needn't reach their ends.
Inputs may be any that keep to these rules, and one draw needn't show every extreme that they name: `counts`: slots past a block's count hold unused values.
All inputs are finite; a program needn't handle non-finite values.
Results may differ from the reference program's by a relative error of at most 0.0012.
Values may be sent and summed in bfloat16 or wider, within the bound.
A program may use at most 64 MiB of HBM per device.

```python
import math
import jax
import jax.numpy as jnp

W = 16384
STRIP = 8
CAP = 192
NROWS = 64
N_GRP = 4
N_OWN = 8


def with_ends(array, rng, low, top_value):
    place = [jax.random.randint(jax.random.fold_in(rng, axis), (), 0, length) for axis, length in enumerate(array.shape)]
    longest = array.shape.index(max(array.shape))
    neighbour = place[:longest] + [(place[longest] + 1) % array.shape[longest]] + place[longest + 1:]
    return array.at[tuple(place)].set(low).at[tuple(neighbour)].set(top_value)


def level_of(own_key, shape, shards, least, high):
    level = 1.0
    for dim, parts in shards:
        steps = jax.random.uniform(jax.random.fold_in(jax.random.fold_in(own_key, 6), dim), (parts,), jnp.float32, least / len(shards), high / len(shards))
        level = level * jnp.repeat(jnp.exp(steps), shape[dim] // parts).reshape((-1,) + (1,) * (len(shape) - 1 - dim))
    return level


def setup_inputs(seed: int = 0) -> dict:
    seeds = jax.random.split(jax.random.key(seed), 6)
    return {
        "tile_row": with_ends(jax.random.randint(seeds[0], (N_GRP, N_OWN, N_OWN * CAP), 0, STRIP), jax.random.fold_in(seeds[0], 1), 0, STRIP - 1).astype(jnp.int32),
        "pixel_col": with_ends(jax.random.randint(seeds[1], (N_GRP, N_OWN, N_OWN * CAP), 0, W), jax.random.fold_in(seeds[1], 1), 0, W - 1).astype(jnp.int32),
        "weight": jnp.clip(jnp.exp(math.log(4.0) - 2.7725887 * jax.random.uniform(seeds[2], (N_GRP, N_OWN, N_OWN * CAP), jnp.float32) ** level_of(seeds[2], (N_GRP, N_OWN, N_OWN * CAP), ((0, 4), (1, 8)), -0.2, 0.2)), 0.25, 4.0).astype(jnp.bfloat16),
        "counts": with_ends(jax.random.randint(seeds[3], (N_GRP, N_OWN, N_OWN), 1, CAP + 1), jax.random.fold_in(seeds[3], 1), 1, CAP).astype(jnp.int32),
        "kernel": jnp.clip(jax.random.uniform(seeds[4], (9, 9), jnp.float32, 0.01, 0.05), 0.01, 0.05),
    }


def reference(tile_row, pixel_col, weight, counts, kernel):
    slot_count = tile_row.shape[2]
    slot_ids = jnp.arange(slot_count, dtype=jnp.int32)
    dest_ids = slot_ids // CAP
    live = (slot_ids % CAP)[None, None, :] < jnp.repeat(counts, CAP, axis=2)
    grid_row = dest_ids[None, None, :] * STRIP + tile_row
    flat_index = (grid_row * W + pixel_col).astype(jnp.int32).reshape(-1)
    values = jnp.where(live, weight.astype(jnp.float32), jnp.zeros((), jnp.float32)).reshape(-1)
    heat = jax.ops.segment_sum(values, flat_index, num_segments=NROWS * W).reshape(NROWS, W)
    padded = jnp.pad(heat, 4)
    smoothed = jnp.zeros((NROWS, W), jnp.float32)
    for a in range(9):
        for b in range(9):
            smoothed = smoothed + kernel[a, b] * padded[a:a + NROWS, b:b + W]
    return smoothed
```

```python
import functools
import math

import jax
import jax.numpy as jnp
from jax import lax
from jax.experimental import pallas as pl
from jax.experimental.pallas import tpu as pltpu
from jax.sharding import PartitionSpec as P

W = 16384
STRIP = 8
REACH = 4
TAPS = 9
LANES = 128
DEEP = 16
BATCHES = (8,)
CHUNK = 1024
MESH = pl.DeviceIdType.MESH


def heat_kernel(
    n_g, n_o, cap, span, row_hbm, col_hbm, weight_hbm, counts_hbm, kern_hbm, out_ref,
    row_ref, col_ref, weight_ref, counts_ref, kern_ref,
    stage, recv, acc, halo_out, halo_in, frame, edge, edge_taps,
    load_sem, send_sem, recv_sem, halo_send_sem, halo_recv_sem,
):
    n = n_g * n_o
    cores = 2 if n_o % 2 == 0 else 1
    me_g, me_o = lax.axis_index("grp"), lax.axis_index("own")
    quarter = out_ref.shape[1]
    slots = row_ref.shape[2]
    tiles = acc.shape[0] // STRIP

    loads = [
        pltpu.make_async_copy(source, target, load_sem.at[k])
        for k, (source, target) in enumerate(
            [
                (counts_hbm, counts_ref),
                (row_hbm, row_ref),
                (col_hbm, col_ref),
                (weight_hbm, weight_ref),
                (kern_hbm, kern_ref),
            ]
        )
    ]
    for load in loads:
        load.start()

    barrier = pltpu.get_barrier_semaphore()

    def offset_place(mine, step, count):
        if count & (count - 1):
            return lax.rem(mine + step, count)
        place, bit = 0, 1
        while bit < count:
            place = place + bit * lax.rem(lax.div(mine, bit) + lax.div(step, bit), 2)
            bit *= 2
        return place

    def mirrored(step, count):
        return lax.rem(count - step, count) if count & (count - 1) else step

    groups = [offset_place(me_g, jnp.int32(u), n_g) for u in range(n_g)]

    def everyone(act):
        def ring(owner, carry):
            for g in range(n_g):

                @pl.when((owner != me_o) | (me_g != g))
                def _():
                    act(g, owner)

            return carry

        lax.fori_loop(0, n_o, ring, 0)

    everyone(
        lambda g, owner: pl.semaphore_signal(
            barrier, inc=1, device_id=(g, owner), device_id_type=MESH
        )
    )

    for load in loads[:4]:
        load.wait()

    period = math.lcm(cap, 128)
    per = period // cap

    def prepare(k, carry):
        at = pl.ds(pl.multiple_of(k * period, 128), period)
        lane = lax.broadcasted_iota(jnp.int32, (1, period), 1)
        limit = jnp.full((1, period), counts_ref[0, 0, k * per], jnp.int32)
        for j in range(1, per):
            limit = jnp.where(lane >= j * cap, counts_ref[0, 0, k * per + j] + j * cap, limit)
        reach = col_ref[0, :, at] + REACH
        index = (reach // LANES * STRIP + row_ref[0, :, at]) * LANES + reach % LANES
        stage[0:1, at] = index.astype(jnp.float32)
        stage[1:2, at] = jnp.where(lane < limit, weight_ref[0, :, at].astype(jnp.float32), 0.0)
        return carry

    lax.fori_loop(0, slots // period, prepare, 0, unroll=slots // period <= 8)

    def window(owner):
        return pl.ds(pl.multiple_of(lax.div(owner * cap, 128) * 128, 128), span)

    def offset_of(mine, place, count):
        if count & (count - 1):
            return lax.rem(place - mine + count, count)
        return offset_place(mine, place, count)

    def send(g, owner):
        step, u = offset_of(me_o, owner, n_o), offset_of(me_g, jnp.int32(g), n_g)
        there = mirrored(step, n_o) * n_g + mirrored(u, n_g)
        pltpu.make_async_remote_copy(
            src_ref=stage.at[:, window(owner)],
            dst_ref=recv.at[there],
            send_sem=send_sem.at[step * n_g + u],
            recv_sem=recv_sem.at[there],
            device_id=(g, owner),
            device_id_type=MESH,
        ).start()

    def arrival(k):
        return pltpu.make_async_remote_copy(
            src_ref=recv.at[k],
            dst_ref=recv.at[k],
            send_sem=send_sem.at[k],
            recv_sem=recv_sem.at[k],
            device_id=(me_g, me_o),
            device_id_type=MESH,
        )

    pl.semaphore_wait(barrier, n - 1)
    everyone(send)
    recv[0] = stage[:, window(me_o)]

    acc[...] = jnp.zeros_like(acc)
    for k in range(halo_in.shape[0]):
        halo_in_zero = jnp.zeros(halo_in.shape[1:], halo_in.dtype)

        @pl.when(me_o == (0 if k == 0 else n_o - 1))
        def _():
            halo_in[k] = halo_in_zero

    loads[4].wait()
    upper = lax.broadcasted_iota(jnp.int32, (STRIP, 128), 0) < REACH
    for a in range(REACH):
        for b in range(TAPS):
            edge_taps[a * TAPS + b] = jnp.where(upper, kern_ref[a, b], kern_ref[a + REACH + 1, b])
    frame[...] = jnp.zeros_like(frame)
    edge[...] = jnp.zeros_like(edge)

    offset = lax.rem(me_o * cap, 128)
    half = jnp.bfloat16
    middle = acc.shape[0] // 2
    origin = me_g * (quarter // LANES * STRIP) + middle
    paired = cap % 128 == 64 and span == cap + 64

    def merged(points):
        lane = lax.broadcasted_iota(jnp.int32, (2, 128), 1)
        width = span - 128
        out, rest = [], []
        for p in points:
            out.append(jnp.where(offset == 0, p[:, :width], p[:, 128:]))
            rest.append(jnp.where(offset == 0, p[:, width:], p[:, :128]))
        for x, y in zip(rest[::2], rest[1::2]):
            out.append(jnp.where((lane < 64) == (offset == 0), x, pltpu.roll(y, 64, 1)))
        return jnp.concatenate(out, axis=1)

    def masked(p):
        place = lax.broadcasted_iota(jnp.int32, (2, span), 1) - offset
        return jnp.where((place >= 0) & (place < cap), p, 0.0)

    def onehots(points):
        count = points.shape[1]
        index = points[0:1].astype(jnp.int32)
        cell = (index // LANES - origin).astype(jnp.float32).astype(half)
        lane = (index % LANES).astype(jnp.float32).astype(half)
        cell_iota = lax.broadcasted_iota(jnp.int32, (acc.shape[0], count), 0) - middle
        cell_iota = cell_iota.astype(jnp.float32).astype(half)
        lane_iota = lax.broadcasted_iota(jnp.int32, (LANES, count), 0).astype(jnp.float32).astype(half)
        cells = jnp.where(cell_iota == cell, half(1), half(0))
        lanes = jnp.where(lane_iota == lane, points[1:2].astype(half), half(0))
        return cells, lanes

    def take(steps):
        places = [step * n_g + u for step in steps for u in range(n_g)]
        for place in places:
            if not (isinstance(place, int) and place == 0):
                arrival(place).wait_recv()
        points = [recv[place] for place in places]
        if paired and len(points) % 2 == 0:
            points = merged(points)
        else:
            points = jnp.concatenate([masked(p) for p in points], axis=1)
        cells, lanes = onehots(points)
        acc[...] += lax.dot_general(
            cells, lanes, (((1,), (1,)), ((), ())), preferred_element_type=jnp.float32
        )

    if n_o <= 8:
        done = 0
        for count in BATCHES:
            steps = range(done, min(done + count, n_o))
            if steps:
                take(steps)
            done += count
        if done < n_o:
            take(range(done, n_o))
    else:
        take([0])

        def one_step(step, carry):
            take([step])
            return carry

        lax.fori_loop(1, n_o, one_step, 0)

    for t in range(tiles):
        heat = acc[t * STRIP : (t + 1) * STRIP, :]
        halo_out[0, t * REACH : (t + 1) * REACH, :] = heat[STRIP - REACH :].astype(half)
        halo_out[1, t * REACH : (t + 1) * REACH, :] = heat[:REACH].astype(half)

    def halo_copy(side, owner):
        return pltpu.make_async_remote_copy(
            src_ref=halo_out.at[side],
            dst_ref=halo_in.at[side],
            send_sem=halo_send_sem.at[side],
            recv_sem=halo_recv_sem.at[side],
            device_id=(me_g, owner),
            device_id_type=MESH,
        )

    @pl.when(me_o < n_o - 1)
    def _():
        halo_copy(0, me_o + 1).start()

    @pl.when(me_o > 0)
    def _():
        halo_copy(1, me_o - 1).start()

    def sent(k, carry):
        arrival(k).wait_send()
        return carry

    for t in range(tiles):
        frame[t * DEEP + REACH : t * DEEP + REACH + STRIP, :] = acc[t * STRIP : (t + 1) * STRIP, :]

    count = CHUNK // LANES

    def smooth(j, carry):
        top = j * count * DEEP
        rows = [
            jnp.concatenate(
                [frame[pl.ds(top + k * DEEP + a, STRIP), :] for k in range(count + 1)], axis=1
            )
            for a in range(TAPS)
        ]
        total = None
        for b in range(TAPS):
            part = rows[0] * kern_ref[0, b]
            for a in range(1, TAPS):
                part = part + rows[a] * kern_ref[a, b]
            part = part[:, b : b + CHUNK]
            total = part if total is None else total + part
        out_ref[:, pl.ds(pl.multiple_of(j * CHUNK, 128), CHUNK)] = total
        return carry

    lax.fori_loop(0, quarter // CHUNK, smooth, 0)
    lax.fori_loop(1, n, sent, 0)

    @pl.when(me_o > 0)
    def _():
        halo_copy(0, me_o - 1).wait_recv()

    @pl.when(me_o < n_o - 1)
    def _():
        halo_copy(1, me_o + 1).wait_recv()

    for t in range(tiles):
        edge[t * DEEP : t * DEEP + REACH, :] = halo_in[0, t * REACH : (t + 1) * REACH, :].astype(jnp.float32)
        edge[t * DEEP + 2 * REACH - 1 : t * DEEP + 3 * REACH - 1, :] = halo_in[
            1, t * REACH : (t + 1) * REACH, :
        ].astype(jnp.float32)

    def smooth_edge(j, carry):
        at = pl.ds(pl.multiple_of(j * CHUNK, 128), CHUNK)
        top = j * count * DEEP
        rows = [
            jnp.concatenate(
                [edge[pl.ds(top + k * DEEP + a, STRIP), :] for k in range(count + 1)], axis=1
            )
            for a in range(REACH)
        ]
        total = out_ref[:, at]
        for b in range(TAPS):
            part = None
            for a in range(REACH):
                taps = jnp.concatenate([edge_taps[a * TAPS + b]] * (count + 1), axis=1)
                term = rows[a] * taps
                part = term if part is None else part + term
            total = total + part[:, b : b + CHUNK]
        out_ref[:, at] = total
        return carry

    lax.fori_loop(0, quarter // CHUNK, smooth_edge, 0)

    @pl.when(me_o < n_o - 1)
    def _():
        halo_copy(0, me_o + 1).wait_send()

    @pl.when(me_o > 0)
    def _():
        halo_copy(1, me_o - 1).wait_send()


def per_device(tile_row, pixel_col, weight, counts, kernel):
    n_o = lax.axis_size("own")
    n_g = lax.axis_size("grp")
    n = n_g * n_o
    slots = tile_row.shape[2]
    cap = slots // n_o
    quarter = W // n_g
    span = -(-(max(o * cap % 128 for o in range(n_o)) + cap) // 128) * 128
    tiles = -(-(quarter + 2 * REACH) // LANES)
    edge_rows = -(-tiles * REACH // 16) * 16
    vmem = pl.BlockSpec(memory_space=pltpu.VMEM)
    hbm = pl.BlockSpec(memory_space=pltpu.HBM)
    return pl.pallas_call(
        functools.partial(heat_kernel, n_g, n_o, cap, span),
        out_shape=pltpu.VMEM((STRIP, quarter), jnp.float32),
        in_specs=[hbm] * 5,
        out_specs=vmem,
        scratch_shapes=[
            pltpu.VMEM(tile_row.shape, jnp.int32),
            pltpu.VMEM(pixel_col.shape, jnp.int32),
            pltpu.VMEM(weight.shape, weight.dtype),
            pltpu.SMEM(counts.shape, jnp.int32),
            pltpu.SMEM(kernel.shape, jnp.float32),
            pltpu.VMEM((2, slots), jnp.float32),
            pltpu.VMEM((n, 2, span), jnp.float32),
            pltpu.VMEM((tiles * STRIP, LANES), jnp.float32),
            pltpu.VMEM((2, edge_rows, LANES), jnp.bfloat16),
            pltpu.VMEM((2, edge_rows, LANES), jnp.bfloat16),
            pltpu.VMEM((tiles * DEEP, LANES), jnp.float32),
            pltpu.VMEM((tiles * DEEP, LANES), jnp.float32),
            pltpu.VMEM((REACH * TAPS, STRIP, 128), jnp.float32),
            pltpu.SemaphoreType.DMA((5,)),
            pltpu.SemaphoreType.DMA((n,)),
            pltpu.SemaphoreType.DMA((n,)),
            pltpu.SemaphoreType.DMA((2,)),
            pltpu.SemaphoreType.DMA((2,)),
        ],
        compiler_params=pltpu.CompilerParams(collective_id=0, has_side_effects=True),
    )(tile_row, pixel_col, weight, counts, kernel)


def solution(mesh):
    placed = (
        P("grp", "own", None),
        P("grp", "own", None),
        P("grp", "own", None),
        P("grp", "own", None),
        P(),
    )
    return jax.shard_map(
        per_device, mesh=mesh, in_specs=placed, out_specs=P("own", "grp"), check_vma=False
    )
```

```python
import functools

import jax
import jax.numpy as jnp
from jax import lax
from jax.experimental import pallas as pl
from jax.experimental.pallas import tpu as pltpu
from jax.sharding import PartitionSpec as P

W = 16384
STRIP = 8
REACH = 4
TAPS = 9
LANES = 128
CHUNK = 1024
MESH = pl.DeviceIdType.MESH


def heat_kernel(
    n_g, n_o, cap, row_hbm, col_hbm, weight_hbm, counts_hbm, kern_hbm, out_ref,
    row_ref, col_ref, weight_ref, counts_ref, kern_ref,
    stage, recv, recv_next, acc, acc_next, halo_out, halo_in, below, band,
    load_sem, send_sem, recv_sem, next_send_sem, next_recv_sem, halo_send_sem, halo_recv_sem,
):
    n = n_g * n_o
    me_g, me_o = lax.axis_index("grp"), lax.axis_index("own")
    quarter = out_ref.shape[1]
    slots = row_ref.shape[2]
    tiles = acc.shape[0] // STRIP
    half = jnp.bfloat16

    loads = [
        pltpu.make_async_copy(source, target, load_sem.at[k])
        for k, (source, target) in enumerate(
            [
                (counts_hbm, counts_ref),
                (row_hbm, row_ref),
                (col_hbm, col_ref),
                (weight_hbm, weight_ref),
                (kern_hbm, kern_ref),
            ]
        )
    ]
    for load in loads:
        load.start()

    barrier = pltpu.get_barrier_semaphore()

    def offset_place(mine, step, count):
        if count & (count - 1):
            return lax.rem(mine + step, count)
        place, bit = 0, 1
        while bit < count:
            place = place + bit * lax.rem(lax.div(mine, bit) + lax.div(step, bit), 2)
            bit *= 2
        return place

    def offset_of(mine, place, count):
        if count & (count - 1):
            return lax.rem(place - mine + count, count)
        return offset_place(mine, place, count)

    def mirrored(step, count):
        return lax.rem(count - step, count) if count & (count - 1) else step

    def everyone(act):
        def ring(owner, carry):
            for g in range(n_g):

                @pl.when((owner != me_o) | (me_g != g))
                def _():
                    act(g, owner)

            return carry

        lax.fori_loop(0, n_o, ring, 0)

    everyone(
        lambda g, owner: pl.semaphore_signal(
            barrier, inc=1, device_id=(g, owner), device_id_type=MESH
        )
    )

    for load in loads[:4]:
        load.wait()

    low = lax.broadcasted_iota(jnp.int32, (1, 128), 1) < 64

    def prepare(k, carry):
        lane = lax.broadcasted_iota(jnp.int32, (1, 128), 1)
        codes, masses = [], []
        for v in range(3):
            at = pl.ds(pl.multiple_of(k * 2 * cap + v * 128, 128), 128)
            reach = col_ref[0, :, at] + REACH
            code = (reach // LANES * STRIP + row_ref[0, :, at]) * LANES + reach % LANES
            codes.append(code.astype(jnp.float32))
            first, second = counts_ref[0, 0, 2 * k], counts_ref[0, 0, 2 * k + 1]
            slot = lane + v * 128
            live = slot < jnp.where(slot < cap, first, second + cap)
            masses.append(jnp.where(live, weight_ref[0, :, at].astype(jnp.float32), 0.0))
        stage[2 * k, :, 0:128] = codes[0]
        stage[2 * k, :, 128:256] = masses[0]
        stage[2 * k, :, 256:384] = jnp.where(low, codes[1], pltpu.roll(masses[1], 64, 1))
        stage[2 * k + 1, :, 0:128] = codes[2]
        stage[2 * k + 1, :, 128:256] = masses[2]
        stage[2 * k + 1, :, 256:384] = jnp.where(low, pltpu.roll(codes[1], 64, 1), masses[1])
        return carry

    lax.fori_loop(0, n_o // 2, prepare, 0, unroll=n_o <= 8)

    def send(source, target, sends, recvs):
        def act(g, owner):
            step, u = offset_of(me_o, owner, n_o), offset_of(me_g, jnp.int32(g), n_g)
            there = mirrored(step, n_o) * n_g + mirrored(u, n_g)
            pltpu.make_async_remote_copy(
                src_ref=stage.at[source(owner)],
                dst_ref=target.at[there],
                send_sem=sends.at[step * n_g + u],
                recv_sem=recvs.at[there],
                device_id=(g, owner),
                device_id_type=MESH,
            ).start()

        return act

    def arrival(k):
        return pltpu.make_async_remote_copy(
            src_ref=recv.at[k],
            dst_ref=recv.at[k],
            send_sem=send_sem.at[k],
            recv_sem=recv_sem.at[k],
            device_id=(me_g, me_o),
            device_id_type=MESH,
        )

    def next_arrival(k):
        return pltpu.make_async_remote_copy(
            src_ref=recv_next.at[k],
            dst_ref=recv_next.at[k],
            send_sem=next_send_sem.at[k],
            recv_sem=next_recv_sem.at[k],
            device_id=(me_g, me_o),
            device_id_type=MESH,
        )

    def reads_next(owner):
        return (lax.rem(owner, 2) == 1) & (owner < n_o - 1)

    pl.semaphore_wait(barrier, n - 1)
    everyone(send(lambda owner: owner, recv, send_sem, recv_sem))
    send_next = send(lambda owner: owner + 1, recv_next, next_send_sem, next_recv_sem)

    def next_ring(k, carry):
        owner = 2 * k + 1
        for g in range(n_g):

            @pl.when((owner != me_o) | (me_g != g))
            def _():
                send_next(g, owner)

        return carry

    lax.fori_loop(0, n_o // 2 - 1, next_ring, 0)
    recv[0] = stage[me_o]

    @pl.when(reads_next(me_o))
    def _():
        recv_next[0] = stage[me_o + 1]

    loads[4].wait()

    spot = lax.broadcasted_iota(jnp.int32, (STRIP, 128), 1)
    line = lax.rem(spot, 2 * STRIP)
    line = jnp.where(line < STRIP, line, jnp.where(line < STRIP + REACH, line - STRIP - REACH, line - REACH))
    tap = line - lax.broadcasted_iota(jnp.int32, (STRIP, 128), 0) + REACH
    for b in range(TAPS):
        taps = jnp.zeros((STRIP, 128), jnp.float32)
        for a in range(TAPS):
            taps = jnp.where(tap == a, kern_ref[a, b], taps)
        coarse = taps.astype(half).astype(jnp.float32)
        band[b * STRIP : (b + 1) * STRIP, :] = jnp.where(spot < 4 * STRIP, coarse, taps - coarse)

    for side, edge in ((0, 0), (1, n_o - 1)):

        @pl.when(me_o == edge)
        def _(side=side):
            halo_in[side] = jnp.zeros(halo_in.shape[1:], half)

    origin = me_g * (quarter // LANES * STRIP)

    def merged(points):
        codes, masses = [], []
        for x, y in zip(points[::2], points[1::2]):
            codes += [x[:, 0:128], y[:, 0:128]]
            masses += [x[:, 128:256], y[:, 128:256]]
            x, y = x[:, 256:384], y[:, 256:384]
            codes.append(jnp.where(low, x, pltpu.roll(y, 64, 1)))
            masses.append(jnp.where(low, pltpu.roll(x, 64, 1), y))
        return jnp.concatenate(codes, axis=1), jnp.concatenate(masses, axis=1)

    def binned(points, rows):
        code, mass = merged(points)
        count = code.shape[1]
        middle = tiles * STRIP // 2
        code = code.astype(jnp.int32)
        cell = (code // LANES - (origin + middle)).astype(jnp.float32).astype(half)
        lane = (code % LANES).astype(jnp.float32).astype(half)
        place = lax.broadcasted_iota(jnp.int32, (tiles * rows, count), 0)
        place = place // rows * STRIP + place % rows - middle
        lane_iota = lax.broadcasted_iota(jnp.int32, (LANES, count), 0).astype(jnp.float32).astype(half)
        cells = jnp.where(place.astype(jnp.float32).astype(half) == cell, half(1), half(0))
        lanes = jnp.where(lane_iota == lane, mass.astype(half), half(0))
        return lax.dot_general(
            cells, lanes, (((1,), (1,)), ((), ())), preferred_element_type=jnp.float32
        )

    def take(source, arrive, target, rows):
        if n_o <= 8:
            for k in range(1, n):
                arrive(k).wait_recv()
            target[...] = binned([source[k] for k in range(n)], rows)
        else:
            target[...] = jnp.zeros_like(target)

            def one_step(step, carry):
                for u in range(n_g):

                    @pl.when(step * n_g + u > 0)
                    def _(u=u):
                        arrive(step * n_g + u).wait_recv()

                target[...] += binned([source[step * n_g + u] for u in range(n_g)], rows)
                return carry

            lax.fori_loop(0, n_o, one_step, 0)

    take(recv, arrival, acc, STRIP)

    for t in range(tiles):
        at = pl.ds(t * LANES, LANES)
        heat = acc[t * STRIP : (t + 1) * STRIP, :]
        halo_out[0, :, at] = heat[STRIP - REACH :].astype(half)
        halo_out[1, :, at] = heat[:REACH].astype(half)

    def halo_copy(side, owner):
        return pltpu.make_async_remote_copy(
            src_ref=halo_out.at[side],
            dst_ref=halo_in.at[side],
            send_sem=halo_send_sem.at[side],
            recv_sem=halo_recv_sem.at[side],
            device_id=(me_g, owner),
            device_id_type=MESH,
        )

    even = lax.rem(me_o, 2) == 0
    sends_down, sends_up = me_o < n_o - 1, lax.rem(me_o, 2) == 1

    @pl.when(sends_down)
    def _():
        halo_copy(0, me_o + 1).start()

    @pl.when(sends_up)
    def _():
        halo_copy(1, me_o - 1).start()

    @pl.when(reads_next(me_o))
    def _():
        take(recv_next, next_arrival, acc_next, REACH)
        for t in range(tiles):
            below[:, t * LANES : (t + 1) * LANES] = acc_next[t * REACH : (t + 1) * REACH, :]

    @pl.when(even)
    def _():
        halo_copy(1, me_o + 1).wait_recv()

    @pl.when(even | (me_o == n_o - 1))
    def _():
        below[...] = halo_in[1].astype(jnp.float32)

    @pl.when(me_o > 0)
    def _():
        halo_copy(0, me_o - 1).wait_recv()

    bands = band[...].astype(half)[:, : 8 * STRIP]
    count = CHUNK // LANES

    for j in range(quarter // CHUNK):
        at = slice(j * CHUNK, (j + 1) * CHUNK + LANES)
        heat = jnp.concatenate(
            [acc[t * STRIP : (t + 1) * STRIP, :] for t in range(j * count, (j + 1) * count + 1)], axis=1
        )
        around = jnp.concatenate([halo_in[0, :, at].astype(jnp.float32), below[:, at]], axis=0)
        field = jnp.concatenate([heat, around], axis=0)
        coarse = field.astype(half)
        fine = (field - coarse.astype(jnp.float32)).astype(half)
        parts = lax.dot_general(
            bands,
            jnp.concatenate([coarse, fine, coarse, fine], axis=0),
            (((1,), (0,)), ((), ())),
            preferred_element_type=jnp.float32,
        )
        total = None
        for b in range(TAPS):
            part = parts[b * STRIP : (b + 1) * STRIP, b : b + CHUNK]
            total = part if total is None else total + part
        out_ref[:, j * CHUNK : (j + 1) * CHUNK] = total

    def sent(k, carry):
        arrival(k).wait_send()
        return carry

    lax.fori_loop(1, n, sent, 0)

    def next_sent(k, carry):
        owner = 2 * k + 1
        for g in range(n_g):

            @pl.when((owner != me_o) | (me_g != g))
            def _():
                step, u = offset_of(me_o, owner, n_o), offset_of(me_g, jnp.int32(g), n_g)
                next_arrival(step * n_g + u).wait_send()

        return carry

    lax.fori_loop(0, n_o // 2 - 1, next_sent, 0)

    @pl.when(sends_down)
    def _():
        halo_copy(0, me_o + 1).wait_send()

    @pl.when(sends_up)
    def _():
        halo_copy(1, me_o - 1).wait_send()


def per_device(tile_row, pixel_col, weight, counts, kernel):
    n_o = lax.axis_size("own")
    n_g = lax.axis_size("grp")
    n = n_g * n_o
    slots = tile_row.shape[2]
    cap = slots // n_o
    quarter = W // n_g
    assert cap == 128 + 64 and n_o % 2 == 0 and n_g % 2 == 0 and quarter % CHUNK == 0
    tiles = -(-(quarter + 2 * REACH) // LANES)
    width = tiles * LANES
    vmem = pl.BlockSpec(memory_space=pltpu.VMEM)
    hbm = pl.BlockSpec(memory_space=pltpu.HBM)
    return pl.pallas_call(
        functools.partial(heat_kernel, n_g, n_o, cap),
        out_shape=pltpu.VMEM((STRIP, quarter), jnp.float32),
        in_specs=[hbm] * 5,
        out_specs=vmem,
        scratch_shapes=[
            pltpu.VMEM(tile_row.shape, jnp.int32),
            pltpu.VMEM(pixel_col.shape, jnp.int32),
            pltpu.VMEM(weight.shape, weight.dtype),
            pltpu.SMEM(counts.shape, jnp.int32),
            pltpu.SMEM(kernel.shape, jnp.float32),
            pltpu.VMEM((n_o, 1, 2 * cap), jnp.float32),
            pltpu.VMEM((n, 1, 2 * cap), jnp.float32),
            pltpu.VMEM((n, 1, 2 * cap), jnp.float32),
            pltpu.VMEM((tiles * STRIP, LANES), jnp.float32),
            pltpu.VMEM((tiles * REACH, LANES), jnp.float32),
            pltpu.VMEM((2, REACH, width), jnp.bfloat16),
            pltpu.VMEM((2, REACH, width), jnp.bfloat16),
            pltpu.VMEM((REACH, width), jnp.float32),
            pltpu.VMEM((TAPS * STRIP, 128), jnp.float32),
            pltpu.SemaphoreType.DMA((5,)),
            pltpu.SemaphoreType.DMA((n,)),
            pltpu.SemaphoreType.DMA((n,)),
            pltpu.SemaphoreType.DMA((n,)),
            pltpu.SemaphoreType.DMA((n,)),
            pltpu.SemaphoreType.DMA((2,)),
            pltpu.SemaphoreType.DMA((2,)),
        ],
        compiler_params=pltpu.CompilerParams(collective_id=0, has_side_effects=True),
    )(tile_row, pixel_col, weight, counts, kernel)


def solution(mesh):
    placed = (
        P("grp", "own", None),
        P("grp", "own", None),
        P("grp", "own", None),
        P("grp", "own", None),
        P(),
    )
    return jax.shard_map(
        per_device, mesh=mesh, in_specs=placed, out_specs=P("own", "grp"), check_vma=False
    )
```

```python
import functools

import jax
import jax.numpy as jnp
from jax import lax
from jax.experimental import pallas as pl
from jax.experimental.pallas import tpu as pltpu
from jax.sharding import PartitionSpec as P

W = 16384
STRIP = 8
REACH = 4
TAPS = 9
LANES = 128
CHUNK = 1024
MESH = pl.DeviceIdType.MESH


def heat_kernel(
    n_g, n_o, cap, row_hbm, col_hbm, weight_hbm, counts_hbm, kern_hbm, out_ref,
    row_ref, col_ref, weight_ref, counts_ref, kern_ref,
    stage, recv, recv_next, acc, acc_next, halo_out, halo_in, below, band,
    load_sem, send_sem, recv_sem, next_send_sem, next_recv_sem, halo_send_sem, halo_recv_sem,
):
    n = n_g * n_o
    me_g, me_o = lax.axis_index("grp"), lax.axis_index("own")
    quarter = out_ref.shape[1]
    slots = row_ref.shape[2]
    tiles = acc.shape[0] // STRIP
    half = jnp.bfloat16

    loads = [
        pltpu.make_async_copy(source, target, load_sem.at[k])
        for k, (source, target) in enumerate(
            [
                (counts_hbm, counts_ref),
                (row_hbm, row_ref),
                (col_hbm, col_ref),
                (weight_hbm, weight_ref),
                (kern_hbm, kern_ref),
            ]
        )
    ]
    for load in loads:
        load.start()

    barrier = pltpu.get_barrier_semaphore()

    def offset_place(mine, step, count):
        if count & (count - 1):
            return lax.rem(mine + step, count)
        place, bit = 0, 1
        while bit < count:
            place = place + bit * lax.rem(lax.div(mine, bit) + lax.div(step, bit), 2)
            bit *= 2
        return place

    def offset_of(mine, place, count):
        if count & (count - 1):
            return lax.rem(place - mine + count, count)
        return offset_place(mine, place, count)

    def mirrored(step, count):
        return lax.rem(count - step, count) if count & (count - 1) else step

    def everyone(act):
        def ring(owner, carry):
            for g in range(n_g):

                @pl.when((owner != me_o) | (me_g != g))
                def _():
                    act(g, owner)

            return carry

        lax.fori_loop(0, n_o, ring, 0)

    everyone(
        lambda g, owner: pl.semaphore_signal(
            barrier, inc=1, device_id=(g, owner), device_id_type=MESH
        )
    )

    for load in loads[:4]:
        load.wait()

    low = lax.broadcasted_iota(jnp.int32, (1, 128), 1) < 64

    def prepare(k, carry):
        lane = lax.broadcasted_iota(jnp.int32, (1, 128), 1)
        codes, masses = [], []
        for v in range(3):
            at = pl.ds(pl.multiple_of(k * 2 * cap + v * 128, 128), 128)
            reach = col_ref[0, :, at] + REACH
            code = (reach // LANES * STRIP + row_ref[0, :, at]) * LANES + reach % LANES
            codes.append(code.astype(jnp.float32))
            first, second = counts_ref[0, 0, 2 * k], counts_ref[0, 0, 2 * k + 1]
            slot = lane + v * 128
            live = slot < jnp.where(slot < cap, first, second + cap)
            masses.append(jnp.where(live, weight_ref[0, :, at].astype(jnp.float32), 0.0))
        stage[2 * k, :, 0:128] = codes[0]
        stage[2 * k, :, 128:256] = masses[0]
        stage[2 * k, :, 256:384] = jnp.where(low, codes[1], pltpu.roll(masses[1], 64, 1))
        stage[2 * k + 1, :, 0:128] = codes[2]
        stage[2 * k + 1, :, 128:256] = masses[2]
        stage[2 * k + 1, :, 256:384] = jnp.where(low, pltpu.roll(codes[1], 64, 1), masses[1])
        return carry

    lax.fori_loop(0, n_o // 2, prepare, 0, unroll=n_o <= 8)

    def send(source, target, sends, recvs):
        def act(g, owner):
            step, u = offset_of(me_o, owner, n_o), offset_of(me_g, jnp.int32(g), n_g)
            there = mirrored(step, n_o) * n_g + mirrored(u, n_g)
            pltpu.make_async_remote_copy(
                src_ref=stage.at[source(owner)],
                dst_ref=target.at[there],
                send_sem=sends,
                recv_sem=recvs,
                device_id=(g, owner),
                device_id_type=MESH,
            ).start()

        return act

    def all_of(target, count, sends, recvs):
        return pltpu.make_async_remote_copy(
            src_ref=target.at[pl.ds(0, count)],
            dst_ref=target.at[pl.ds(0, count)],
            send_sem=sends,
            recv_sem=recvs,
            device_id=(me_g, me_o),
            device_id_type=MESH,
        )

    arrivals = all_of(recv, n - 1, send_sem, recv_sem)
    next_arrivals = all_of(recv_next, n - 1, next_send_sem, next_recv_sem)

    def reads_next(owner):
        return (lax.rem(owner, 2) == 1) & (owner < n_o - 1)

    pl.semaphore_wait(barrier, n - 1)
    everyone(send(lambda owner: owner, recv, send_sem, recv_sem))
    send_next = send(lambda owner: owner + 1, recv_next, next_send_sem, next_recv_sem)

    def next_ring(k, carry):
        owner = 2 * k + 1
        for g in range(n_g):

            @pl.when((owner != me_o) | (me_g != g))
            def _():
                send_next(g, owner)

        return carry

    lax.fori_loop(0, n_o // 2 - 1, next_ring, 0)
    recv[0] = stage[me_o]

    @pl.when(reads_next(me_o))
    def _():
        recv_next[0] = stage[me_o + 1]

    loads[4].wait()

    spot = lax.broadcasted_iota(jnp.int32, (STRIP, 128), 1)
    line = lax.rem(spot, 2 * STRIP)
    line = jnp.where(line < STRIP, line, jnp.where(line < STRIP + REACH, line - STRIP - REACH, line - REACH))
    tap = line - lax.broadcasted_iota(jnp.int32, (STRIP, 128), 0) + REACH
    for b in range(TAPS):
        taps = jnp.zeros((STRIP, 128), jnp.float32)
        for a in range(TAPS):
            taps = jnp.where(tap == a, kern_ref[a, b], taps)
        coarse = taps.astype(half).astype(jnp.float32)
        band[b * STRIP : (b + 1) * STRIP, :] = jnp.where(spot < 4 * STRIP, coarse, taps - coarse)

    for side, edge in ((0, 0), (1, n_o - 1)):

        @pl.when(me_o == edge)
        def _(side=side):
            halo_in[side] = jnp.zeros(halo_in.shape[1:], half)

    origin = me_g * (quarter // LANES * STRIP)

    def merged(points):
        codes, masses = [], []
        for x, y in zip(points[::2], points[1::2]):
            codes += [x[:, 0:128], y[:, 0:128]]
            masses += [x[:, 128:256], y[:, 128:256]]
            x, y = x[:, 256:384], y[:, 256:384]
            codes.append(jnp.where(low, x, pltpu.roll(y, 64, 1)))
            masses.append(jnp.where(low, pltpu.roll(x, 64, 1), y))
        return jnp.concatenate(codes, axis=1), jnp.concatenate(masses, axis=1)

    def binned(points, rows):
        code, mass = merged(points)
        count = code.shape[1]
        middle = tiles * STRIP // 2
        code = code.astype(jnp.int32)
        cell = (code // LANES - (origin + middle)).astype(jnp.float32).astype(half)
        lane = (code % LANES).astype(jnp.float32).astype(half)
        place = lax.broadcasted_iota(jnp.int32, (tiles * rows, count), 0)
        place = place // rows * STRIP + place % rows - middle
        lane_iota = lax.broadcasted_iota(jnp.int32, (LANES, count), 0).astype(jnp.float32).astype(half)
        cells = jnp.where(place.astype(jnp.float32).astype(half) == cell, half(1), half(0))
        lanes = jnp.where(lane_iota == lane, mass.astype(half), half(0))
        return lax.dot_general(
            cells, lanes, (((1,), (1,)), ((), ())), preferred_element_type=jnp.float32
        )

    def take(source, target, rows):
        if n_o <= 8:
            target[...] = binned([source[k] for k in range(n)], rows)
        else:
            target[...] = jnp.zeros_like(target)

            def one_step(step, carry):
                target[...] += binned([source[step * n_g + u] for u in range(n_g)], rows)
                return carry

            lax.fori_loop(0, n_o, one_step, 0)

    arrivals.wait_recv()
    take(recv, acc, STRIP)

    for t in range(tiles):
        at = pl.ds(t * LANES, LANES)
        heat = acc[t * STRIP : (t + 1) * STRIP, :]
        halo_out[0, :, at] = heat[STRIP - REACH :].astype(half)
        halo_out[1, :, at] = heat[:REACH].astype(half)

    def halo_copy(side, owner):
        return pltpu.make_async_remote_copy(
            src_ref=halo_out.at[side],
            dst_ref=halo_in.at[side],
            send_sem=halo_send_sem.at[side],
            recv_sem=halo_recv_sem.at[side],
            device_id=(me_g, owner),
            device_id_type=MESH,
        )

    even = lax.rem(me_o, 2) == 0
    sends_down, sends_up = me_o < n_o - 1, lax.rem(me_o, 2) == 1

    @pl.when(sends_down)
    def _():
        halo_copy(0, me_o + 1).start()

    @pl.when(sends_up)
    def _():
        halo_copy(1, me_o - 1).start()

    @pl.when(reads_next(me_o))
    def _():
        next_arrivals.wait_recv()
        take(recv_next, acc_next, REACH)
        for t in range(tiles):
            below[:, t * LANES : (t + 1) * LANES] = acc_next[t * REACH : (t + 1) * REACH, :]

    @pl.when(even)
    def _():
        halo_copy(1, me_o + 1).wait_recv()

    @pl.when(even | (me_o == n_o - 1))
    def _():
        below[...] = halo_in[1].astype(jnp.float32)

    @pl.when(me_o > 0)
    def _():
        halo_copy(0, me_o - 1).wait_recv()

    bands = band[...].astype(half)[:, : 8 * STRIP]
    count = CHUNK // LANES

    for j in range(quarter // CHUNK):
        at = slice(j * CHUNK, (j + 1) * CHUNK + LANES)
        heat = jnp.concatenate(
            [acc[t * STRIP : (t + 1) * STRIP, :] for t in range(j * count, (j + 1) * count + 1)], axis=1
        )
        around = jnp.concatenate([halo_in[0, :, at].astype(jnp.float32), below[:, at]], axis=0)
        field = jnp.concatenate([heat, around], axis=0)
        coarse = field.astype(half)
        fine = (field - coarse.astype(jnp.float32)).astype(half)
        parts = lax.dot_general(
            bands,
            jnp.concatenate([coarse, fine, coarse, fine], axis=0),
            (((1,), (0,)), ((), ())),
            preferred_element_type=jnp.float32,
        )
        total = None
        for b in range(TAPS):
            part = parts[b * STRIP : (b + 1) * STRIP, b : b + CHUNK]
            total = part if total is None else total + part
        out_ref[:, j * CHUNK : (j + 1) * CHUNK] = total

    arrivals.wait_send()
    readers = n_g * (n_o // 2 - 1)

    @pl.when(reads_next(me_o))
    def _():
        all_of(recv_next, readers - 1, next_send_sem, next_recv_sem).wait_send()

    @pl.when(jnp.logical_not(reads_next(me_o)))
    def _():
        all_of(recv_next, readers, next_send_sem, next_recv_sem).wait_send()

    @pl.when(sends_down)
    def _():
        halo_copy(0, me_o + 1).wait_send()

    @pl.when(sends_up)
    def _():
        halo_copy(1, me_o - 1).wait_send()


def per_device(tile_row, pixel_col, weight, counts, kernel):
    n_o = lax.axis_size("own")
    n_g = lax.axis_size("grp")
    n = n_g * n_o
    slots = tile_row.shape[2]
    cap = slots // n_o
    quarter = W // n_g
    assert cap == 128 + 64 and n_o % 2 == 0 and n_g % 2 == 0 and quarter % CHUNK == 0
    tiles = -(-(quarter + 2 * REACH) // LANES)
    width = tiles * LANES
    vmem = pl.BlockSpec(memory_space=pltpu.VMEM)
    hbm = pl.BlockSpec(memory_space=pltpu.HBM)
    return pl.pallas_call(
        functools.partial(heat_kernel, n_g, n_o, cap),
        out_shape=pltpu.VMEM((STRIP, quarter), jnp.float32),
        in_specs=[hbm] * 5,
        out_specs=vmem,
        scratch_shapes=[
            pltpu.VMEM(tile_row.shape, jnp.int32),
            pltpu.VMEM(pixel_col.shape, jnp.int32),
            pltpu.VMEM(weight.shape, weight.dtype),
            pltpu.SMEM(counts.shape, jnp.int32),
            pltpu.SMEM(kernel.shape, jnp.float32),
            pltpu.VMEM((n_o, 1, 2 * cap), jnp.float32),
            pltpu.VMEM((n, 1, 2 * cap), jnp.float32),
            pltpu.VMEM((n, 1, 2 * cap), jnp.float32),
            pltpu.VMEM((tiles * STRIP, LANES), jnp.float32),
            pltpu.VMEM((tiles * REACH, LANES), jnp.float32),
            pltpu.VMEM((2, REACH, width), jnp.bfloat16),
            pltpu.VMEM((2, REACH, width), jnp.bfloat16),
            pltpu.VMEM((REACH, width), jnp.float32),
            pltpu.VMEM((TAPS * STRIP, 128), jnp.float32),
            pltpu.SemaphoreType.DMA((5,)),
            pltpu.SemaphoreType.DMA,
            pltpu.SemaphoreType.DMA,
            pltpu.SemaphoreType.DMA,
            pltpu.SemaphoreType.DMA,
            pltpu.SemaphoreType.DMA((2,)),
            pltpu.SemaphoreType.DMA((2,)),
        ],
        compiler_params=pltpu.CompilerParams(collective_id=0, has_side_effects=True),
    )(tile_row, pixel_col, weight, counts, kernel)


def solution(mesh):
    placed = (
        P("grp", "own", None),
        P("grp", "own", None),
        P("grp", "own", None),
        P("grp", "own", None),
        P(),
    )
    return jax.shard_map(
        per_device, mesh=mesh, in_specs=placed, out_specs=P("own", "grp"), check_vma=False
    )
```

```python
import functools

import jax
import jax.numpy as jnp
from jax import lax
from jax.experimental import pallas as pl
from jax.experimental.pallas import tpu as pltpu
from jax.sharding import PartitionSpec as P

W = 16384
STRIP = 8
REACH = 4
TAPS = 9
LANES = 128
CHUNK = 1024
MESH = pl.DeviceIdType.MESH


def hops_of(g, n_g):
    total, bit = 0, 1
    while bit < n_g:
        total, bit = total + g // bit % 2, bit * 2
    return total


def heat_kernel(
    n_g, n_o, cap, late, row_hbm, col_hbm, weight_hbm, counts_hbm, kern_hbm, out_ref,
    row_ref, col_ref, weight_ref, counts_ref, kern_ref,
    stage, recv, recv_late, acc, acc_side, halo_out, halo_in, band,
    ready, load_sem, send_sem, recv_sem, late_sem, halo_send_sem, halo_recv_sem,
):
    n = n_g * n_o
    me_g, me_o = lax.axis_index("grp"), lax.axis_index("own")
    quarter = out_ref.shape[1]
    slots = row_ref.shape[2]
    tiles = acc.shape[0] // STRIP
    half = jnp.bfloat16
    side = lax.rem(me_o, 2)

    loads = [
        pltpu.make_async_copy(source, target, load_sem.at[k])
        for k, (source, target) in enumerate(
            [
                (counts_hbm, counts_ref),
                (row_hbm, row_ref),
                (col_hbm, col_ref),
                (weight_hbm, weight_ref),
                (kern_hbm, kern_ref),
            ]
        )
    ]
    for load in loads:
        load.start()

    barrier = pltpu.get_barrier_semaphore()

    def key(g, owner, hops):
        return (hops + lax.div(owner, 2)) * n + owner * n_g + g

    mine = key(me_g, me_o, hops_of(me_g, n_g))

    def everyone(act):
        def ring(owner, carry):
            for g in range(n_g):
                act(g, owner, key(g, owner, hops_of(g, n_g)))
            return carry

        lax.fori_loop(0, n_o, ring, 0)

    def count_earlier(owner, count):
        for g in range(n_g):
            count = count + jnp.where(key(g, owner, hops_of(g, n_g)) < mine, 1, 0)
        return count

    def tell(semaphore, wanted):
        def act(g, owner, other):
            @pl.when(wanted(other))
            def _():
                pl.semaphore_signal(
                    semaphore, inc=1, device_id=(g, owner), device_id_type=MESH
                )

        return act

    everyone(tell(barrier, lambda other: other > mine))
    earlier = lax.fori_loop(0, n_o, count_earlier, jnp.int32(0))

    @pl.when(earlier > 0)
    def _():
        pl.semaphore_wait(barrier, earlier)

    everyone(tell(ready, lambda other: other < mine))

    for load in loads[:4]:
        load.wait()

    low = lax.broadcasted_iota(jnp.int32, (1, 128), 1) < 64

    def prepare(k, carry):
        lane = lax.broadcasted_iota(jnp.int32, (1, 128), 1)
        codes, masses = [], []
        for v in range(3):
            at = pl.ds(pl.multiple_of(k * 2 * cap + v * 128, 128), 128)
            reach = col_ref[0, :, at] + REACH
            code = (reach // LANES * STRIP + row_ref[0, :, at]) * LANES + reach % LANES
            codes.append(code.astype(jnp.float32))
            first, second = counts_ref[0, 0, 2 * k], counts_ref[0, 0, 2 * k + 1]
            slot = lane + v * 128
            live = slot < jnp.where(slot < cap, first, second + cap)
            masses.append(jnp.where(live, weight_ref[0, :, at].astype(jnp.float32), 0.0))
        stage[2 * k + 1, :, 0:128] = codes[0]
        stage[2 * k + 1, :, 128:256] = masses[0]
        stage[2 * k + 1, :, 256:384] = jnp.where(low, codes[1], pltpu.roll(masses[1], 64, 1))
        stage[2 * k + 2, :, 0:128] = codes[2]
        stage[2 * k + 2, :, 128:256] = masses[2]
        stage[2 * k + 2, :, 256:384] = jnp.where(low, pltpu.roll(codes[1], 64, 1), masses[1])
        return carry

    lax.fori_loop(0, n_o // 2, prepare, 0, unroll=n_o <= 8)

    for k in (0, n_o + 1):
        stage[k] = jnp.zeros(stage.shape[1:], jnp.float32)

    spot = me_o * n_g + me_g
    lately = functools.reduce(jnp.logical_or, [spot == k for k in late], False) if late else None

    def pair_of(owner):
        return pl.ds(owner + lax.rem(owner, 2), 2)

    def trio_of(owner):
        return pl.ds(owner, 3)

    def send(window, target, arrived):
        def act(g, owner):
            pltpu.make_async_remote_copy(
                src_ref=stage.at[window(owner)],
                dst_ref=target.at[spot],
                send_sem=send_sem,
                recv_sem=arrived,
                device_id=(g, owner),
                device_id_type=MESH,
            ).start()

        return act

    def when_late(yes, no):
        if lately is None:
            no()
        else:
            pl.when(lately)(yes)
            pl.when(jnp.logical_not(lately))(no)

    def send_to(wanted):
        def loop(act):
            def one(g, owner, other):
                @pl.when(wanted(other))
                def _():
                    act(g, owner)

            everyone(one)

        when_late(
            lambda: loop(send(trio_of, recv_late, late_sem)),
            lambda: loop(send(pair_of, recv, recv_sem)),
        )

    def all_of(target, count):
        return pltpu.make_async_remote_copy(
            src_ref=target.at[pl.ds(0, count)],
            dst_ref=target.at[pl.ds(0, count)],
            send_sem=send_sem,
            recv_sem=recv_sem if target is recv else late_sem,
            device_id=(me_g, me_o),
            device_id_type=MESH,
        )

    send_to(lambda other: other < mine)

    def keep_late():
        recv_late[spot] = stage[trio_of(me_o)]

    def keep():
        recv[spot] = stage[pair_of(me_o)]

    when_late(keep_late, keep)

    @pl.when(earlier < n - 1)
    def _():
        pl.semaphore_wait(ready, n - 1 - earlier)

    send_to(lambda other: other > mine)

    loads[4].wait()

    column = lax.broadcasted_iota(jnp.int32, (STRIP, 128), 1)
    line = lax.rem(column, 2 * STRIP)
    line = jnp.where(line < STRIP, line, jnp.where(line < STRIP + REACH, line - STRIP - REACH, line - REACH))
    tap = line - lax.broadcasted_iota(jnp.int32, (STRIP, 128), 0) + REACH
    for b in range(TAPS):
        taps = jnp.zeros((STRIP, 128), jnp.float32)
        for a in range(TAPS):
            taps = jnp.where(tap == a, kern_ref[a, b], taps)
        coarse = taps.astype(half).astype(jnp.float32)
        band[b * STRIP : (b + 1) * STRIP, :] = jnp.where(column < 4 * STRIP, coarse, taps - coarse)

    origin = me_g * (quarter // LANES * STRIP)

    def merged(points):
        codes, masses = [], []
        for x, y in zip(points[::2], points[1::2]):
            codes += [x[:, 0:128], y[:, 0:128]]
            masses += [x[:, 128:256], y[:, 128:256]]
            x, y = x[:, 256:384], y[:, 256:384]
            codes.append(jnp.where(low, x, pltpu.roll(y, 64, 1)))
            masses.append(jnp.where(low, pltpu.roll(x, 64, 1), y))
        return jnp.concatenate(codes, axis=1), jnp.concatenate(masses, axis=1)

    def binned(points, rows, base=0):
        code, mass = merged(points)
        count = code.shape[1]
        middle = tiles * STRIP // 2
        code = code.astype(jnp.int32)
        cell = (code // LANES - (origin + middle + base)).astype(jnp.float32).astype(half)
        lane = (code % LANES).astype(jnp.float32).astype(half)
        place = lax.broadcasted_iota(jnp.int32, (tiles * rows, count), 0)
        place = place // rows * STRIP + place % rows - middle
        lane_iota = lax.broadcasted_iota(jnp.int32, (LANES, count), 0).astype(jnp.float32).astype(half)
        cells = jnp.where(place.astype(jnp.float32).astype(half) == cell, half(1), half(0))
        lanes = jnp.where(lane_iota == lane, mass.astype(half), half(0))
        return lax.dot_general(
            cells, lanes, (((1,), (1,)), ((), ())), preferred_element_type=jnp.float32
        )

    early = [k for k in range(n) if k not in late]

    def take(target, rows, which, base):
        if n_o <= 8:
            target[...] = binned([recv[k, which] for k in early], rows, base)
        else:
            target[...] = jnp.zeros_like(target)

            def one_step(step, carry):
                target[...] += binned([recv[step * n_g + g, which] for g in range(n_g)], rows, base)
                return carry

            lax.fori_loop(0, n_o, one_step, 0)

    when_late(
        lambda: all_of(recv, len(early)).wait_recv(), lambda: all_of(recv, len(early) - 1).wait_recv()
    )
    take(acc, STRIP, 1 - side, 0)

    for t in range(tiles):
        heat = acc[t * STRIP : (t + 1) * STRIP, :]
        edge = jnp.where(side == 0, heat[STRIP - REACH :], heat[:REACH])
        halo_out[:, t * LANES : (t + 1) * LANES] = edge.astype(half)
    halo = pltpu.make_async_remote_copy(
        src_ref=halo_out,
        dst_ref=halo_in,
        send_sem=halo_send_sem,
        recv_sem=halo_recv_sem,
        device_id=(me_g, me_o + 1 - 2 * side),
        device_id_type=MESH,
    )
    halo.start()

    outermost = (me_o == 0) | (me_o == n_o - 1)

    @pl.when(outermost)
    def _():
        acc_side[...] = jnp.zeros_like(acc_side)

    @pl.when(jnp.logical_not(outermost))
    def _():
        take(acc_side, REACH, side, REACH * (1 - side))

    if late:
        when_late(
            lambda: all_of(recv_late, len(late) - 1).wait_recv() if len(late) > 1 else None,
            lambda: all_of(recv_late, len(late)).wait_recv(),
        )
        acc[...] += binned([recv_late[k, 1] for k in late], STRIP)
        above = binned([recv_late[k, 0] for k in late], REACH, REACH)
        below = binned([recv_late[k, 2] for k in late], REACH)
    halo.wait_recv()

    bands = band[...].astype(half)[:, : 8 * STRIP]
    count = CHUNK // LANES
    fields = []
    for t in range(tiles):
        at, rows = slice(t * LANES, (t + 1) * LANES), slice(t * REACH, (t + 1) * REACH)
        mate, other = halo_in[:, at].astype(jnp.float32), acc_side[rows, :]
        around = jnp.concatenate(
            [jnp.where(side == 0, other, mate), jnp.where(side == 0, mate, other)], axis=0
        )
        if late:
            around = around + jnp.concatenate([above[rows], below[rows]], axis=0)
        fields.append(jnp.concatenate([acc[t * STRIP : (t + 1) * STRIP, :], around], axis=0))

    for j in range(quarter // CHUNK):
        field = jnp.concatenate(fields[j * count : (j + 1) * count + 1], axis=1)
        coarse = field.astype(half)
        fine = (field - coarse.astype(jnp.float32)).astype(half)
        parts = lax.dot_general(
            bands,
            jnp.concatenate([coarse, fine, coarse, fine], axis=0),
            (((1,), (0,)), ((), ())),
            preferred_element_type=jnp.float32,
        )
        total = None
        for b in range(TAPS):
            part = parts[b * STRIP : (b + 1) * STRIP, b : b + CHUNK]
            total = part if total is None else total + part
        out_ref[:, j * CHUNK : (j + 1) * CHUNK] = total

    when_late(
        lambda: all_of(recv_late, n - 1).wait_send(), lambda: all_of(recv, n - 1).wait_send()
    )
    halo.wait_send()


def per_device(tile_row, pixel_col, weight, counts, kernel):
    n_o = lax.axis_size("own")
    n_g = lax.axis_size("grp")
    n = n_g * n_o
    slots = tile_row.shape[2]
    cap = slots // n_o
    quarter = W // n_g
    assert cap == 128 + 64 and n_o % 2 == 0 and n_g % 2 == 0 and quarter % CHUNK == 0
    tiles = -(-(quarter + 2 * REACH) // LANES)
    width = tiles * LANES
    hops = [hops_of(k % n_g, n_g) + k // n_g // 2 for k in range(n)]
    late = [k for k in range(n) if hops[k] == max(hops)] if n_o <= 8 else []
    vmem = pl.BlockSpec(memory_space=pltpu.VMEM)
    hbm = pl.BlockSpec(memory_space=pltpu.HBM)
    return pl.pallas_call(
        functools.partial(heat_kernel, n_g, n_o, cap, late),
        out_shape=pltpu.VMEM((STRIP, quarter), jnp.float32),
        in_specs=[hbm] * 5,
        out_specs=vmem,
        scratch_shapes=[
            pltpu.VMEM(tile_row.shape, jnp.int32),
            pltpu.VMEM(pixel_col.shape, jnp.int32),
            pltpu.VMEM(weight.shape, weight.dtype),
            pltpu.SMEM(counts.shape, jnp.int32),
            pltpu.SMEM(kernel.shape, jnp.float32),
            pltpu.VMEM((n_o + 2, 1, 2 * cap), jnp.float32),
            pltpu.VMEM((n, 2, 1, 2 * cap), jnp.float32),
            pltpu.VMEM((n if late else 1, 3, 1, 2 * cap), jnp.float32),
            pltpu.VMEM((tiles * STRIP, LANES), jnp.float32),
            pltpu.VMEM((tiles * REACH, LANES), jnp.float32),
            pltpu.VMEM((REACH, width), jnp.bfloat16),
            pltpu.VMEM((REACH, width), jnp.bfloat16),
            pltpu.VMEM((TAPS * STRIP, 128), jnp.float32),
            pltpu.SemaphoreType.REGULAR,
            pltpu.SemaphoreType.DMA((5,)),
            pltpu.SemaphoreType.DMA,
            pltpu.SemaphoreType.DMA,
            pltpu.SemaphoreType.DMA,
            pltpu.SemaphoreType.DMA,
            pltpu.SemaphoreType.DMA,
        ],
        compiler_params=pltpu.CompilerParams(collective_id=0, has_side_effects=True),
    )(tile_row, pixel_col, weight, counts, kernel)


def solution(mesh):
    placed = (
        P("grp", "own", None),
        P("grp", "own", None),
        P("grp", "own", None),
        P("grp", "own", None),
        P(),
    )
    return jax.shard_map(
        per_device, mesh=mesh, in_specs=placed, out_specs=P("own", "grp"), check_vma=False
    )
```

```python
import functools

import jax
import jax.numpy as jnp
from jax import lax
from jax.experimental import pallas as pl
from jax.experimental.pallas import tpu as pltpu
from jax.sharding import PartitionSpec as P

W = 16384
STRIP = 8
REACH = 4
TAPS = 9
LANES = 128
CHUNK = 1024
MESH = pl.DeviceIdType.MESH
DOWN = False


def hops_of(g, n_g):
    total, bit = 0, 1
    while bit < n_g:
        total, bit = total + g // bit % 2, bit * 2
    return total


def heat_kernel(
    n_g, n_o, cap, late, row_hbm, col_hbm, weight_hbm, counts_hbm, kern_hbm, out_ref,
    row_ref, col_ref, weight_ref, counts_ref, kern_ref,
    stage, recv, recv_side, recv_late, acc, acc_side, halo_out, halo_in, band,
    ready, load_sem, send_sem, recv_sem, side_send_sem, side_recv_sem, late_sem, halo_send_sem, halo_recv_sem,
):
    n = n_g * n_o
    me_g, me_o = lax.axis_index("grp"), lax.axis_index("own")
    side = lax.rem(me_o, 2)
    quarter = out_ref.shape[1]
    slots = row_ref.shape[2]
    tiles = acc.shape[0] // STRIP
    half = jnp.bfloat16

    loads = [
        pltpu.make_async_copy(source, target, load_sem.at[k])
        for k, (source, target) in enumerate(
            [
                (counts_hbm, counts_ref),
                (row_hbm, row_ref),
                (col_hbm, col_ref),
                (weight_hbm, weight_ref),
                (kern_hbm, kern_ref),
            ]
        )
    ]
    for load in loads:
        load.start()

    barrier = pltpu.get_barrier_semaphore()

    early = [k for k in range(n) if k not in late]
    spot = me_o * n_g + me_g
    none = me_o < 0
    my_chip = lax.div(me_o, 2)

    def bits(g):
        return [lax.rem(lax.div(g, 1 << b), 2) for b in range(n_g.bit_length() - 1)]

    def covered(g, by):
        if n_g & (n_g - 1):
            return g <= by
        return functools.reduce(jnp.logical_and, [x <= y for x, y in zip(bits(jnp.int32(g)), bits(by))], me_o >= 0)

    inner = [covered(g, me_g) for g in range(n_g)]
    outer = [covered(me_g, jnp.int32(g)) for g in range(n_g)]
    same = [me_g == g for g in range(n_g)]

    def precedes(g, owner):
        chip = lax.div(owner, 2)
        return inner[g] & ((chip < my_chip) | ((chip == my_chip) & (jnp.logical_not(same[g]) | (owner < me_o))))

    def follows(g, owner):
        chip = lax.div(owner, 2)
        return outer[g] & ((chip > my_chip) | ((chip == my_chip) & (jnp.logical_not(same[g]) | (owner > me_o))))

    def the_rest(g, owner):
        return jnp.logical_not(precedes(g, owner) | (same[g] & (owner == me_o)))

    lately = functools.reduce(jnp.logical_or, [spot == k for k in late], none)

    def when_late(yes, no):
        if late:
            pl.when(lately)(yes)
            pl.when(jnp.logical_not(lately))(no)
        else:
            no()

    def visit(act, wanted, low, high, down=False):
        def chip(i, carry):
            z = low + high - 1 - i if down else i
            for g in range(n_g):
                for c in range(2):
                    owner = 2 * z + c

                    @pl.when(wanted(g, owner))
                    def _(g=g, owner=owner):
                        act(g, owner)

            return carry

        lax.fori_loop(low, high, chip, 0)

    def to_earlier(act, also=lambda owner: owner >= 0):
        visit(act, lambda g, o: precedes(g, o) & also(o), 0, my_chip + 1)

    def to_others(act, also=lambda owner: owner >= 0):
        visit(act, lambda g, o: the_rest(g, o) & also(o), 0, n_o // 2, DOWN)

    def tell(semaphore):
        return lambda g, owner: pl.semaphore_signal(
            semaphore, inc=1, device_id=(g, owner), device_id_type=MESH
        )

    visit(tell(barrier), follows, my_chip, n_o // 2)

    def count(owner, counts):
        before, after = counts
        for g in range(n_g):
            before = before + jnp.where(precedes(g, owner), 1, 0)
            after = after + jnp.where(follows(g, owner), 1, 0)
        return before, after

    earlier, later = lax.fori_loop(0, n_o, count, (jnp.int32(0), jnp.int32(0)), unroll=n_o <= 8)

    @pl.when(earlier > 0)
    def _():
        pl.semaphore_wait(barrier, earlier)

    to_earlier(tell(ready))

    for load in loads[:4]:
        load.wait()

    low = lax.broadcasted_iota(jnp.int32, (1, 128), 1) < 64

    def prepare(k, carry):
        lane = lax.broadcasted_iota(jnp.int32, (1, 128), 1)
        codes, masses = [], []
        for v in range(3):
            at = pl.ds(pl.multiple_of(k * 2 * cap + v * 128, 128), 128)
            reach = col_ref[0, :, at] + REACH
            code = (reach // LANES * STRIP + row_ref[0, :, at]) * LANES + reach % LANES
            codes.append(code.astype(jnp.float32))
            first, second = counts_ref[0, 0, 2 * k], counts_ref[0, 0, 2 * k + 1]
            slot = lane + v * 128
            live = slot < jnp.where(slot < cap, first, second + cap)
            masses.append(jnp.where(live, weight_ref[0, :, at].astype(jnp.float32), 0.0))
        stage[2 * k + 1, :, 0:128] = codes[0]
        stage[2 * k + 1, :, 128:256] = masses[0]
        stage[2 * k + 1, :, 256:384] = jnp.where(low, codes[1], pltpu.roll(masses[1], 64, 1))
        stage[2 * k + 2, :, 0:128] = codes[2]
        stage[2 * k + 2, :, 128:256] = masses[2]
        stage[2 * k + 2, :, 256:384] = jnp.where(low, pltpu.roll(codes[1], 64, 1), masses[1])
        return carry

    lax.fori_loop(0, n_o // 2, prepare, 0, unroll=n_o <= 8)

    for k in (0, n_o + 1):
        stage[k] = jnp.zeros(stage.shape[1:], jnp.float32)

    def send(source, target, sends, recvs):
        return lambda g, owner: pltpu.make_async_remote_copy(
            src_ref=stage.at[source(owner)],
            dst_ref=target.at[spot],
            send_sem=sends,
            recv_sem=recvs,
            device_id=(g, owner),
            device_id_type=MESH,
        ).start()

    def trio_of(owner):
        return pl.ds(owner, 3)

    def all_of(target, count, sends, recvs):
        return pltpu.make_async_remote_copy(
            src_ref=target.at[pl.ds(0, count)],
            dst_ref=target.at[pl.ds(0, count)],
            send_sem=sends,
            recv_sem=recvs,
            device_id=(me_g, me_o),
            device_id_type=MESH,
        )

    def reads_side(owner):
        return (owner > 0) & (owner < n_o - 1)

    send_own = send(lambda owner: owner + 1, recv, send_sem, recv_sem)
    send_side = send(lambda owner: owner + 2 * lax.rem(owner, 2), recv_side, side_send_sem, side_recv_sem)
    send_trio = send(trio_of, recv_late, send_sem, late_sem)

    when_late(
        lambda: to_earlier(send_trio),
        lambda: (to_earlier(send_own), to_earlier(send_side, reads_side))[0],
    )

    def keep_late():
        recv_late[spot] = stage[trio_of(me_o)]

    def keep_early():
        recv[spot] = stage[me_o + 1]

        @pl.when(reads_side(me_o))
        def _():
            recv_side[spot] = stage[me_o + 2 * side]

    when_late(keep_late, keep_early)

    @pl.when(later > 0)
    def _():
        pl.semaphore_wait(ready, later)

    when_late(
        lambda: to_others(send_trio),
        lambda: (to_others(send_own), to_others(send_side, reads_side))[0],
    )

    loads[4].wait()

    spot = lax.broadcasted_iota(jnp.int32, (STRIP, 128), 1)
    line = lax.rem(spot, 2 * STRIP)
    line = jnp.where(line < STRIP, line, jnp.where(line < STRIP + REACH, line - STRIP - REACH, line - REACH))
    tap = line - lax.broadcasted_iota(jnp.int32, (STRIP, 128), 0) + REACH
    for b in range(TAPS):
        taps = jnp.zeros((STRIP, 128), jnp.float32)
        for a in range(TAPS):
            taps = jnp.where(tap == a, kern_ref[a, b], taps)
        coarse = taps.astype(half).astype(jnp.float32)
        band[b * STRIP : (b + 1) * STRIP, :] = jnp.where(spot < 4 * STRIP, coarse, taps - coarse)

    origin = me_g * (quarter // LANES * STRIP)

    def merged(points):
        codes, masses = [], []
        for x, y in zip(points[::2], points[1::2]):
            codes += [x[:, 0:128], y[:, 0:128]]
            masses += [x[:, 128:256], y[:, 128:256]]
            x, y = x[:, 256:384], y[:, 256:384]
            codes.append(jnp.where(low, x, pltpu.roll(y, 64, 1)))
            masses.append(jnp.where(low, pltpu.roll(x, 64, 1), y))
        return jnp.concatenate(codes, axis=1), jnp.concatenate(masses, axis=1)

    def binned(points, rows, base=0):
        code, mass = merged(points)
        count = code.shape[1]
        middle = tiles * STRIP // 2
        code = code.astype(jnp.int32)
        cell = (code // LANES - (origin + middle + base)).astype(jnp.float32).astype(half)
        lane = (code % LANES).astype(jnp.float32).astype(half)
        place = lax.broadcasted_iota(jnp.int32, (tiles * rows, count), 0)
        place = place // rows * STRIP + place % rows - middle
        lane_iota = lax.broadcasted_iota(jnp.int32, (LANES, count), 0).astype(jnp.float32).astype(half)
        cells = jnp.where(place.astype(jnp.float32).astype(half) == cell, half(1), half(0))
        lanes = jnp.where(lane_iota == lane, mass.astype(half), half(0))
        return lax.dot_general(
            cells, lanes, (((1,), (1,)), ((), ())), preferred_element_type=jnp.float32
        )

    def take(source, target, rows, base=0):
        if n_o <= 8:
            target[...] = binned([source[k] for k in early], rows, base)
        else:
            target[...] = jnp.zeros_like(target)

            def one_step(step, carry):
                target[...] += binned([source[step * n_g + u] for u in range(n_g)], rows, base)
                return carry

            lax.fori_loop(0, n_o, one_step, 0)

    when_late(
        lambda: all_of(recv, len(early), send_sem, recv_sem).wait_recv(),
        lambda: all_of(recv, len(early) - 1, send_sem, recv_sem).wait_recv(),
    )
    take(recv, acc, STRIP)

    for t in range(tiles):
        heat = acc[t * STRIP : (t + 1) * STRIP, :]
        edge = jnp.where(side == 0, heat[STRIP - REACH :], heat[:REACH])
        halo_out[:, t * LANES : (t + 1) * LANES] = edge.astype(half)
    halo = pltpu.make_async_remote_copy(
        src_ref=halo_out,
        dst_ref=halo_in,
        send_sem=halo_send_sem,
        recv_sem=halo_recv_sem,
        device_id=(me_g, me_o + 1 - 2 * side),
        device_id_type=MESH,
    )
    halo.start()

    @pl.when(reads_side(me_o))
    def _():
        when_late(
            lambda: all_of(recv_side, len(early), side_send_sem, side_recv_sem).wait_recv(),
            lambda: all_of(recv_side, len(early) - 1, side_send_sem, side_recv_sem).wait_recv(),
        )
        take(recv_side, acc_side, REACH, REACH * (1 - side))

    @pl.when(jnp.logical_not(reads_side(me_o)))
    def _():
        acc_side[...] = jnp.zeros_like(acc_side)

    if late:

        def wait_late():
            if len(late) > 1:
                all_of(recv_late, len(late) - 1, send_sem, late_sem).wait_recv()

        when_late(wait_late, lambda: all_of(recv_late, len(late), send_sem, late_sem).wait_recv())
        acc[...] += binned([recv_late[k, 1] for k in late], STRIP)
        late_above = binned([recv_late[k, 0] for k in late], REACH, REACH)
        late_below = binned([recv_late[k, 2] for k in late], REACH)

    halo.wait_recv()
    fields = []
    for t in range(tiles):
        at, rows = slice(t * LANES, (t + 1) * LANES), slice(t * REACH, (t + 1) * REACH)
        mate, other = halo_in[:, at].astype(jnp.float32), acc_side[rows, :]
        around = jnp.concatenate(
            [jnp.where(side == 0, other, mate), jnp.where(side == 0, mate, other)], axis=0
        )
        if late:
            around = around + jnp.concatenate([late_above[rows], late_below[rows]], axis=0)
        fields.append(jnp.concatenate([acc[t * STRIP : (t + 1) * STRIP, :], around], axis=0))

    bands = band[...].astype(half)[:, : 8 * STRIP]
    count = CHUNK // LANES

    for j in range(quarter // CHUNK):
        field = jnp.concatenate(fields[j * count : (j + 1) * count + 1], axis=1)
        coarse = field.astype(half)
        fine = (field - coarse.astype(jnp.float32)).astype(half)
        parts = lax.dot_general(
            bands,
            jnp.concatenate([coarse, fine, coarse, fine], axis=0),
            (((1,), (0,)), ((), ())),
            preferred_element_type=jnp.float32,
        )
        total = None
        for b in range(TAPS):
            part = parts[b * STRIP : (b + 1) * STRIP, b : b + CHUNK]
            total = part if total is None else total + part
        out_ref[:, j * CHUNK : (j + 1) * CHUNK] = total

    readers = n_g * (n_o - 2)

    def finish_early():
        all_of(recv, n - 1, send_sem, recv_sem).wait_send()

        @pl.when(reads_side(me_o))
        def _():
            all_of(recv_side, readers - 1, side_send_sem, side_recv_sem).wait_send()

        @pl.when(jnp.logical_not(reads_side(me_o)))
        def _():
            all_of(recv_side, readers, side_send_sem, side_recv_sem).wait_send()

    when_late(lambda: all_of(recv_late, n - 1, send_sem, late_sem).wait_send(), finish_early)
    halo.wait_send()


def per_device(tile_row, pixel_col, weight, counts, kernel):
    n_o = lax.axis_size("own")
    n_g = lax.axis_size("grp")
    n = n_g * n_o
    slots = tile_row.shape[2]
    cap = slots // n_o
    quarter = W // n_g
    assert cap == 128 + 64 and n_o % 2 == 0 and n_g % 2 == 0 and quarter % CHUNK == 0
    tiles = -(-(quarter + 2 * REACH) // LANES)
    width = tiles * LANES
    hops = [hops_of(k % n_g, n_g) + k // n_g // 2 for k in range(n)]
    late = [k for k in range(n) if hops[k] == max(hops)] if n_o <= 8 else []
    vmem = pl.BlockSpec(memory_space=pltpu.VMEM)
    hbm = pl.BlockSpec(memory_space=pltpu.HBM)
    return pl.pallas_call(
        functools.partial(heat_kernel, n_g, n_o, cap, late),
        out_shape=pltpu.VMEM((STRIP, quarter), jnp.float32),
        in_specs=[hbm] * 5,
        out_specs=vmem,
        scratch_shapes=[
            pltpu.VMEM(tile_row.shape, jnp.int32),
            pltpu.VMEM(pixel_col.shape, jnp.int32),
            pltpu.VMEM(weight.shape, weight.dtype),
            pltpu.SMEM(counts.shape, jnp.int32),
            pltpu.SMEM(kernel.shape, jnp.float32),
            pltpu.VMEM((n_o + 2, 1, 2 * cap), jnp.float32),
            pltpu.VMEM((n, 1, 2 * cap), jnp.float32),
            pltpu.VMEM((n, 1, 2 * cap), jnp.float32),
            pltpu.VMEM((n if late else 1, 3, 1, 2 * cap), jnp.float32),
            pltpu.VMEM((tiles * STRIP, LANES), jnp.float32),
            pltpu.VMEM((tiles * REACH, LANES), jnp.float32),
            pltpu.VMEM((REACH, width), jnp.bfloat16),
            pltpu.VMEM((REACH, width), jnp.bfloat16),
            pltpu.VMEM((TAPS * STRIP, 128), jnp.float32),
            pltpu.SemaphoreType.REGULAR,
            pltpu.SemaphoreType.DMA((5,)),
            pltpu.SemaphoreType.DMA,
            pltpu.SemaphoreType.DMA,
            pltpu.SemaphoreType.DMA,
            pltpu.SemaphoreType.DMA,
            pltpu.SemaphoreType.DMA,
            pltpu.SemaphoreType.DMA,
            pltpu.SemaphoreType.DMA,
        ],
        compiler_params=pltpu.CompilerParams(collective_id=0, has_side_effects=True),
    )(tile_row, pixel_col, weight, counts, kernel)


def solution(mesh):
    placed = (
        P("grp", "own", None),
        P("grp", "own", None),
        P("grp", "own", None),
        P("grp", "own", None),
        P(),
    )
    return jax.shard_map(
        per_device, mesh=mesh, in_specs=placed, out_specs=P("own", "grp"), check_vma=False
    )
```

```python
import functools

import jax
import jax.numpy as jnp
from jax import lax
from jax.experimental import pallas as pl
from jax.experimental.pallas import tpu as pltpu
from jax.sharding import PartitionSpec as P

W = 16384
STRIP = 8
REACH = 4
TAPS = 9
LANES = 128
CHUNK = 1024
MESH = pl.DeviceIdType.MESH


def hops_of(g, n_g):
    total, bit = 0, 1
    while bit < n_g:
        total, bit = total + g // bit % 2, bit * 2
    return total


def heat_kernel(
    n_g, n_o, cap, late, row_hbm, col_hbm, weight_hbm, counts_hbm, kern_hbm, out_ref,
    row_ref, col_ref, weight_ref, counts_ref, kern_ref,
    stage, recv, recv_side, recv_late, acc, acc_side, acc_mate, halo_out, halo_in, band,
    ready, load_sem, send_sem, recv_sem, side_send_sem, side_recv_sem, late_sem, halo_send_sem, halo_recv_sem,
):
    n = n_g * n_o
    me_g, me_o = lax.axis_index("grp"), lax.axis_index("own")
    side = lax.rem(me_o, 2)
    quarter = out_ref.shape[1]
    slots = row_ref.shape[2]
    tiles = acc.shape[0] // STRIP
    half = jnp.bfloat16

    loads = [
        pltpu.make_async_copy(source, target, load_sem.at[k])
        for k, (source, target) in enumerate(
            [
                (counts_hbm, counts_ref),
                (row_hbm, row_ref),
                (col_hbm, col_ref),
                (weight_hbm, weight_ref),
                (kern_hbm, kern_ref),
            ]
        )
    ]
    for load in loads:
        load.start()

    barrier = pltpu.get_barrier_semaphore()

    early = [k for k in range(n) if k not in late]
    spot = me_o * n_g + me_g
    none = me_o < 0
    my_chip = lax.div(me_o, 2)

    def bits(g):
        return [lax.rem(lax.div(g, 1 << b), 2) for b in range(n_g.bit_length() - 1)]

    def covered(g, by):
        if n_g & (n_g - 1):
            return g <= by
        return functools.reduce(jnp.logical_and, [x <= y for x, y in zip(bits(jnp.int32(g)), bits(by))], me_o >= 0)

    inner = [covered(g, me_g) for g in range(n_g)]
    outer = [covered(me_g, jnp.int32(g)) for g in range(n_g)]
    same = [me_g == g for g in range(n_g)]

    one_if = lambda flag: jnp.where(flag, 1, 0)
    chips = n_o // 2
    before = [jnp.where(inner[g], my_chip + 1 - one_if(same[g]), 0) for g in range(n_g)]
    after = [jnp.where(outer[g], my_chip + one_if(same[g]), chips) for g in range(n_g)]
    rest = [jnp.where(inner[g], my_chip + 1, 0) for g in range(n_g)]
    earlier = 2 * sum(before) + side
    later = 2 * sum(chips - start for start in after) + 1 - side
    mate = me_o + 1 - 2 * side

    lately = functools.reduce(jnp.logical_or, [spot == k for k in late], none)

    def when_late(yes, no):
        if late:
            pl.when(lately)(yes)
            pl.when(jnp.logical_not(lately))(no)
        else:
            no()

    def visit(act, lows, highs, with_mate):
        def chip(z, carry):
            for g in range(n_g):

                @pl.when((z >= lows[g]) & (z < highs[g]))
                def _(g=g):
                    for c in range(2):
                        act(g, 2 * z + c)

            return carry

        lax.fori_loop(0, chips, chip, 0)

        @pl.when(with_mate)
        def _():
            act(me_g, mate)

    def to_earlier(act):
        visit(act, [0] * n_g, before, side == 1)

    def to_others(act):
        visit(act, rest, [chips] * n_g, side == 0)

    def tell(semaphore):
        return lambda g, owner: pl.semaphore_signal(
            semaphore, inc=1, device_id=(g, owner), device_id_type=MESH
        )

    visit(tell(barrier), after, [chips] * n_g, side == 0)

    @pl.when(earlier > 0)
    def _():
        pl.semaphore_wait(barrier, earlier)

    to_earlier(tell(ready))

    for load in loads[:4]:
        load.wait()

    low = lax.broadcasted_iota(jnp.int32, (1, 128), 1) < 64

    def prepare(k, carry):
        lane = lax.broadcasted_iota(jnp.int32, (1, 128), 1)
        codes, masses = [], []
        for v in range(3):
            at = pl.ds(pl.multiple_of(k * 2 * cap + v * 128, 128), 128)
            reach = col_ref[0, :, at] + REACH
            code = (reach // LANES * STRIP + row_ref[0, :, at]) * LANES + reach % LANES
            codes.append(code.astype(jnp.float32))
            first, second = counts_ref[0, 0, 2 * k], counts_ref[0, 0, 2 * k + 1]
            slot = lane + v * 128
            live = slot < jnp.where(slot < cap, first, second + cap)
            masses.append(jnp.where(live, weight_ref[0, :, at].astype(jnp.float32), 0.0))
        stage[2 * k + 1, :, 0:128] = codes[0]
        stage[2 * k + 1, :, 128:256] = masses[0]
        stage[2 * k + 1, :, 256:384] = jnp.where(low, codes[1], pltpu.roll(masses[1], 64, 1))
        stage[2 * k + 2, :, 0:128] = codes[2]
        stage[2 * k + 2, :, 128:256] = masses[2]
        stage[2 * k + 2, :, 256:384] = jnp.where(low, pltpu.roll(codes[1], 64, 1), masses[1])
        return carry

    lax.fori_loop(0, n_o // 2, prepare, 0, unroll=n_o <= 8)

    for k in (0, n_o + 1):
        stage[k] = jnp.zeros(stage.shape[1:], jnp.float32)

    def send(source, target, sends, recvs):
        return lambda g, owner: pltpu.make_async_remote_copy(
            src_ref=stage.at[source(owner)],
            dst_ref=target.at[spot],
            send_sem=sends,
            recv_sem=recvs,
            device_id=(g, owner),
            device_id_type=MESH,
        ).start()

    def trio_of(owner):
        return pl.ds(owner, 3)

    def all_of(target, count, sends, recvs):
        return pltpu.make_async_remote_copy(
            src_ref=target.at[pl.ds(0, count)],
            dst_ref=target.at[pl.ds(0, count)],
            send_sem=sends,
            recv_sem=recvs,
            device_id=(me_g, me_o),
            device_id_type=MESH,
        )

    def reads_side(owner):
        return (owner > 0) & (owner < n_o - 1)

    send_own = send(lambda owner: owner + 1, recv, send_sem, recv_sem)
    send_side = send(lambda owner: owner + 2 * lax.rem(owner, 2), recv_side, side_send_sem, side_recv_sem)

    def send_beside(g, owner):
        @pl.when(reads_side(owner))
        def _():
            send_side(g, owner)

    send_trio = send(trio_of, recv_late, send_sem, late_sem)

    when_late(
        lambda: to_earlier(send_trio),
        lambda: (to_earlier(send_own), to_earlier(send_beside))[0],
    )

    def keep_late():
        recv_late[spot] = stage[trio_of(me_o)]

    def keep_early():
        recv[spot] = stage[me_o + 1]

        @pl.when(reads_side(me_o))
        def _():
            recv_side[spot] = stage[me_o + 2 * side]

    when_late(keep_late, keep_early)

    @pl.when(later > 0)
    def _():
        pl.semaphore_wait(ready, later)

    when_late(
        lambda: to_others(send_trio),
        lambda: (to_others(send_own), to_others(send_beside))[0],
    )

    loads[4].wait()

    spot = lax.broadcasted_iota(jnp.int32, (STRIP, 128), 1)
    line = lax.rem(spot, 2 * STRIP)
    line = jnp.where(line < STRIP, line, jnp.where(line < STRIP + REACH, line - STRIP - REACH, line - REACH))
    tap = line - lax.broadcasted_iota(jnp.int32, (STRIP, 128), 0) + REACH
    for b in range(TAPS):
        taps = jnp.zeros((STRIP, 128), jnp.float32)
        for a in range(TAPS):
            taps = jnp.where(tap == a, kern_ref[a, b], taps)
        coarse = taps.astype(half).astype(jnp.float32)
        band[b * STRIP : (b + 1) * STRIP, :] = jnp.where(spot < 4 * STRIP, coarse, taps - coarse)

    acc_mate[...] = jnp.zeros_like(acc_mate)

    @pl.when(jnp.logical_not(reads_side(me_o)))
    def _():
        acc_side[...] = jnp.zeros_like(acc_side)

    origin = me_g * (quarter // LANES * STRIP)

    def merged(points):
        codes, masses = [], []
        for x, y in zip(points[::2], points[1::2]):
            codes += [x[:, 0:128], y[:, 0:128]]
            masses += [x[:, 128:256], y[:, 128:256]]
            x, y = x[:, 256:384], y[:, 256:384]
            codes.append(jnp.where(low, x, pltpu.roll(y, 64, 1)))
            masses.append(jnp.where(low, pltpu.roll(x, 64, 1), y))
        return jnp.concatenate(codes, axis=1), jnp.concatenate(masses, axis=1)

    def binned(points, rows, base=0):
        code, mass = merged(points)
        count = code.shape[1]
        middle = tiles * STRIP // 2
        code = code.astype(jnp.int32)
        cell = (code // LANES - (origin + middle + base)).astype(jnp.float32).astype(half)
        lane = (code % LANES).astype(jnp.float32).astype(half)
        place = lax.broadcasted_iota(jnp.int32, (tiles * rows, count), 0)
        place = place // rows * STRIP + place % rows - middle
        lane_iota = lax.broadcasted_iota(jnp.int32, (LANES, count), 0).astype(jnp.float32).astype(half)
        cells = jnp.where(place.astype(jnp.float32).astype(half) == cell, half(1), half(0))
        lanes = jnp.where(lane_iota == lane, mass.astype(half), half(0))
        return lax.dot_general(
            cells, lanes, (((1,), (1,)), ((), ())), preferred_element_type=jnp.float32
        )

    def take(source, target, rows, base=0, more=()):
        if n_o <= 8:
            target[...] = binned([source[k] for k in early] + [recv_late[k, at] for k, at in more], rows, base)
        else:
            target[...] = jnp.zeros_like(target)

            def one_step(step, carry):
                target[...] += binned([source[step * n_g + u] for u in range(n_g)], rows, base)
                return carry

            lax.fori_loop(0, n_o, one_step, 0)

    first_chip = (me_g == 0) & (me_o < 2)

    def when_first(yes, no):
        if late:
            pl.when(first_chip)(yes)
            pl.when(jnp.logical_not(first_chip))(no)
        else:
            no()

    def wait_late():
        if late:
            when_late(
                lambda: all_of(recv_late, len(late) - 1, send_sem, late_sem).wait_recv() if len(late) > 1 else None,
                lambda: all_of(recv_late, len(late), send_sem, late_sem).wait_recv(),
            )

    when_late(
        lambda: all_of(recv, len(early), send_sem, recv_sem).wait_recv(),
        lambda: all_of(recv, len(early) - 1, send_sem, recv_sem).wait_recv(),
    )

    def take_all():
        wait_late()
        take(recv, acc, STRIP, 0, [(k, 1) for k in late])

    when_first(lambda: take(recv, acc, STRIP), take_all)

    for t in range(tiles):
        heat = acc[t * STRIP : (t + 1) * STRIP, :]
        edge = jnp.where(side == 0, heat[STRIP - REACH :], heat[:REACH])
        halo_out[:, t * LANES : (t + 1) * LANES] = edge.astype(half)
    halo = pltpu.make_async_remote_copy(
        src_ref=halo_out,
        dst_ref=halo_in,
        send_sem=halo_send_sem,
        recv_sem=halo_recv_sem,
        device_id=(me_g, me_o + 1 - 2 * side),
        device_id_type=MESH,
    )
    halo.start()

    @pl.when(reads_side(me_o))
    def _():
        when_late(
            lambda: all_of(recv_side, len(early), side_send_sem, side_recv_sem).wait_recv(),
            lambda: all_of(recv_side, len(early) - 1, side_send_sem, side_recv_sem).wait_recv(),
        )
        base = REACH * (1 - side)
        when_first(
            lambda: take(recv_side, acc_side, REACH, base),
            lambda: take(recv_side, acc_side, REACH, base, [(k, 2 * side) for k in late]),
        )

    if late:

        @pl.when(first_chip)
        def _():
            wait_late()
            acc[...] += binned([recv_late[k, 1] for k in late], STRIP)
            acc_side[...] += binned([recv_late[k, 2 * side] for k in late], REACH, REACH * (1 - side))
            acc_mate[...] = binned([recv_late[k, 2 - 2 * side] for k in late], REACH, REACH * side)

    halo.wait_recv()
    fields = []
    for t in range(tiles):
        at, rows = slice(t * LANES, (t + 1) * LANES), slice(t * REACH, (t + 1) * REACH)
        near, other = halo_in[:, at].astype(jnp.float32) + acc_mate[rows, :], acc_side[rows, :]
        around = jnp.concatenate(
            [jnp.where(side == 0, other, near), jnp.where(side == 0, near, other)], axis=0
        )
        fields.append(jnp.concatenate([acc[t * STRIP : (t + 1) * STRIP, :], around], axis=0))

    bands = band[...].astype(half)[:, : 8 * STRIP]
    count = CHUNK // LANES

    for j in range(quarter // CHUNK):
        field = jnp.concatenate(fields[j * count : (j + 1) * count + 1], axis=1)
        coarse = field.astype(half)
        fine = (field - coarse.astype(jnp.float32)).astype(half)
        parts = lax.dot_general(
            bands,
            jnp.concatenate([coarse, fine, coarse, fine], axis=0),
            (((1,), (0,)), ((), ())),
            preferred_element_type=jnp.float32,
        )
        for k in range(count):
            total = parts[:STRIP, k * LANES : (k + 1) * LANES]
            for b in range(1, TAPS):
                row = parts[b * STRIP : (b + 1) * STRIP, k * LANES : (k + 2) * LANES]
                mixed = jnp.where(spot >= b, row[:, :LANES], row[:, LANES:])
                total = total + pltpu.roll(mixed, LANES - b, 1)
            at = j * CHUNK + k * LANES
            out_ref[:, at : at + LANES] = total

    readers = n_g * (n_o - 2)

    def finish_early():
        all_of(recv, n - 1, send_sem, recv_sem).wait_send()

        @pl.when(reads_side(me_o))
        def _():
            all_of(recv_side, readers - 1, side_send_sem, side_recv_sem).wait_send()

        @pl.when(jnp.logical_not(reads_side(me_o)))
        def _():
            all_of(recv_side, readers, side_send_sem, side_recv_sem).wait_send()

    when_late(lambda: all_of(recv_late, n - 1, send_sem, late_sem).wait_send(), finish_early)
    halo.wait_send()


def per_device(tile_row, pixel_col, weight, counts, kernel):
    n_o = lax.axis_size("own")
    n_g = lax.axis_size("grp")
    n = n_g * n_o
    slots = tile_row.shape[2]
    cap = slots // n_o
    quarter = W // n_g
    assert cap == 128 + 64 and n_o % 2 == 0 and n_g % 2 == 0 and quarter % CHUNK == 0
    tiles = -(-(quarter + 2 * REACH) // LANES)
    width = tiles * LANES
    hops = [hops_of(k % n_g, n_g) + k // n_g // 2 for k in range(n)]
    late = [k for k in range(n) if hops[k] == max(hops)] if n_o <= 8 else []
    vmem = pl.BlockSpec(memory_space=pltpu.VMEM)
    hbm = pl.BlockSpec(memory_space=pltpu.HBM)
    return pl.pallas_call(
        functools.partial(heat_kernel, n_g, n_o, cap, late),
        out_shape=pltpu.VMEM((STRIP, quarter), jnp.float32),
        in_specs=[hbm] * 5,
        out_specs=vmem,
        scratch_shapes=[
            pltpu.VMEM(tile_row.shape, jnp.int32),
            pltpu.VMEM(pixel_col.shape, jnp.int32),
            pltpu.VMEM(weight.shape, weight.dtype),
            pltpu.SMEM(counts.shape, jnp.int32),
            pltpu.SMEM(kernel.shape, jnp.float32),
            pltpu.VMEM((n_o + 2, 1, 2 * cap), jnp.float32),
            pltpu.VMEM((n, 1, 2 * cap), jnp.float32),
            pltpu.VMEM((n, 1, 2 * cap), jnp.float32),
            pltpu.VMEM((n if late else 1, 3, 1, 2 * cap), jnp.float32),
            pltpu.VMEM((tiles * STRIP, LANES), jnp.float32),
            pltpu.VMEM((tiles * REACH, LANES), jnp.float32),
            pltpu.VMEM((tiles * REACH, LANES), jnp.float32),
            pltpu.VMEM((REACH, width), jnp.bfloat16),
            pltpu.VMEM((REACH, width), jnp.bfloat16),
            pltpu.VMEM((TAPS * STRIP, 128), jnp.float32),
            pltpu.SemaphoreType.REGULAR,
            pltpu.SemaphoreType.DMA((5,)),
            pltpu.SemaphoreType.DMA,
            pltpu.SemaphoreType.DMA,
            pltpu.SemaphoreType.DMA,
            pltpu.SemaphoreType.DMA,
            pltpu.SemaphoreType.DMA,
            pltpu.SemaphoreType.DMA,
            pltpu.SemaphoreType.DMA,
        ],
        compiler_params=pltpu.CompilerParams(collective_id=0, has_side_effects=True),
    )(tile_row, pixel_col, weight, counts, kernel)


def solution(mesh):
    placed = (
        P("grp", "own", None),
        P("grp", "own", None),
        P("grp", "own", None),
        P("grp", "own", None),
        P(),
    )
    return jax.shard_map(
        per_device, mesh=mesh, in_specs=placed, out_specs=P("own", "grp"), check_vma=False
    )
```
